32 devices in a mesh: row: 8 (over z, x), col: 4 (over y, core).
Axes of the slice: x: 2, y: 2, z: 4, core: 2. Of those that a mesh axis runs over, the one named last changes fastest.
Arguments:
- visible_data: bfloat16 [512, 32768], P('col', 'row'), may hold values from 0 to 1
- hidden_uniform: float32 [512, 16384], P('row', 'col'), may hold values from 0.01 to 0.99
- visible_uniform: float32 [512, 32768], P('col', 'row'), may hold values from 0.01 to 0.99
- weights: bfloat16 [32768, 16384], P('row', 'col'), may hold values from -0.03125 to 0.03125
- visible_bias: float32 [32768], P('row'), may hold values from -4 to 4
- hidden_bias: float32 [16384], P('col'), may hold values from -4 to 4
Outputs:
- grad_weights: bfloat16 [32768, 16384], P('row', 'col')
- grad_visible: float32 [32768], P('row')
- grad_hidden: float32 [16384], P('col')
- hidden_sample: bfloat16 [512, 16384], P('row', 'col')
- reconstruction: bfloat16 [512, 32768], P('col', 'row')
The draws below stay inside these ranges and needn't reach their ends.
All inputs are finite; a program needn't handle non-finite values.
Results may differ from the reference program's by a relative error of at most 0.0034.
Values may be sent and summed in bfloat16 or wider, within the bound.
A program may use at most 192 MiB of HBM per device.

```python
import jax
import jax.numpy as jnp

V = 32768
H = 16384
BATCH = 512


def block_scale(key, dims, shards, low, largest):
    gain, own = 1.0, jax.random.fold_in(key, 6)
    for dim, blocks in shards:
        draws = jnp.exp(jax.random.uniform(jax.random.fold_in(own, dim), (blocks,), jnp.float32, low / len(shards), largest / len(shards)))
        gain = gain * jnp.repeat(draws, dims[dim] // blocks).reshape([-1 if axis == dim else 1 for axis in range(len(dims))])
    return gain


def noise(rng, extent, spread, bound, cuts=(), dtype=jnp.bfloat16):
    values = jax.random.normal(rng, extent, jnp.float32) * spread
    if len(cuts) > 0:
        values = block_scale(rng, extent, cuts, -0.22, 0.18) * values
    return jnp.clip(values, min=-bound, max=bound).astype(dtype)


def setup_inputs(seed: int = 0) -> dict:
    splits = jax.random.split(jax.random.key(seed), 7)
    visible_data = jnp.clip(1.0 * jax.random.uniform(splits[0], (BATCH, V), jnp.float32) ** block_scale(splits[0], (BATCH, V), ((0, 4), (1, 8)), -0.2, 0.2), 0.0, 1.0).astype(jnp.bfloat16)
    hidden_uniform = jnp.clip(0.01 + 0.98 * jax.random.uniform(splits[1], (BATCH, H), jnp.float32) ** block_scale(splits[1], (BATCH, H), ((0, 8), (1, 4)), -0.2, 0.2), 0.01, 0.99)
    visible_uniform = jnp.clip(0.01 + 0.98 * jax.random.uniform(splits[2], (BATCH, V), jnp.float32) ** block_scale(splits[2], (BATCH, V), ((0, 4), (1, 8)), -0.2, 0.2), 0.01, 0.99)
    weights = noise(splits[3], (V, H), V ** -0.5, 0.03125, ((0, 8), (1, 4)))
    visible_bias = noise(splits[4], (V,), 1.0, 4.0, ((0, 8),), jnp.float32)
    hidden_bias = noise(splits[5], (H,), 1.0, 4.0, ((0, 4),), jnp.float32)
    return {"visible_data": visible_data, "hidden_uniform": hidden_uniform, "visible_uniform": visible_uniform, "weights": weights, "visible_bias": visible_bias, "hidden_bias": hidden_bias}


def relaxed(field, uniform):
    return jax.nn.sigmoid(2.0 * (field + jnp.log(uniform) - jnp.log1p(-uniform)))


def reference(visible_data, hidden_uniform, visible_uniform, weights, visible_bias, hidden_bias):
    field_pos = jnp.dot(visible_data, weights, preferred_element_type=jnp.float32) + hidden_bias
    probs_pos = jax.nn.sigmoid(field_pos).astype(jnp.bfloat16)
    hidden_sample = relaxed(field_pos, hidden_uniform).astype(jnp.bfloat16)
    field_neg = jnp.dot(hidden_sample, weights.T, preferred_element_type=jnp.float32) + visible_bias
    reconstruction = relaxed(field_neg, visible_uniform).astype(jnp.bfloat16)
    field_back = jnp.dot(reconstruction, weights, preferred_element_type=jnp.float32) + hidden_bias
    probs_neg = jax.nn.sigmoid(field_back).astype(jnp.bfloat16)
    positive = jnp.dot(visible_data.T, probs_pos, preferred_element_type=jnp.float32)
    negative = jnp.dot(reconstruction.T, probs_neg, preferred_element_type=jnp.float32)
    grad_weights = ((positive - negative) / BATCH).astype(jnp.bfloat16)
    grad_visible = jnp.mean(visible_data.astype(jnp.float32) - reconstruction.astype(jnp.float32), axis=0)
    grad_hidden = jnp.mean(probs_pos.astype(jnp.float32) - probs_neg.astype(jnp.float32), axis=0)
    return grad_weights, grad_visible, grad_hidden, hidden_sample, reconstruction
```

```python
import functools

import jax
import jax.numpy as jnp
from jax import lax
from jax.experimental import pallas as pl
from jax.experimental.pallas import tpu as pltpu
from jax.sharding import PartitionSpec as P

MESH = pl.DeviceIdType.MESH
BF16 = jnp.bfloat16
F32 = jnp.float32
ANY = pl.BlockSpec(memory_space=pl.ANY)
VM = pl.BlockSpec(memory_space=pltpu.VMEM)
LIMIT = 64_000_000


def sigmoid(t):
    return 1.0 / (1.0 + jnp.exp(-t))


def relaxed(field, uniform):
    return sigmoid(2.0 * (field + jnp.log(uniform) - jnp.log(1.0 - uniform)))


def col_tile(size, want):
    return min(size, want)


class Ring:
    def __init__(self, n):
        self.n = n
        me = lax.axis_index("row")
        self.me = me
        self.col = lax.axis_index("col")
        half, odd = me // 2, me % 2
        self.pos = half + odd * (n - 1 - 2 * half)
        self.right = self.index(self.pos + 1)
        self.left = self.index(self.pos + n - 1)

    def index(self, p):
        p = lax.rem(p, self.n)
        far = p // (self.n // 2)
        return (1 - far) * (2 * p) + far * (2 * (self.n - 1 - p) + 1)

    def peer(self, d):
        return (self.right if d == 0 else self.left, self.col)

    def rs_chunk(self, d, step):
        if d == 0:
            return self.index(self.pos + 2 * self.n - 1 - step)
        return self.index(self.pos + 1 + step)

    def ag_chunk(self, d, step):
        if d == 0:
            return self.index(self.pos + self.n - step)
        return self.index(self.pos + step)


class Group:
    def __init__(self, m):
        self.m = m
        self.chips = m // 2
        self.me = lax.axis_index("col")
        self.row = lax.axis_index("row")
        self.chip, self.core = self.me // 2, self.me % 2
        self.partner = (self.row, 2 * self.chip + 1 - self.core)

    def chip_at(self, offset):
        return lax.rem(self.chip + offset, self.chips)

    def peer(self, offset):
        return (self.row, 2 * self.chip_at(offset) + self.core)


def barrier(devices):
    sem = pltpu.get_barrier_semaphore()
    for device in devices:
        pl.semaphore_signal(sem, inc=1, device_id=device, device_id_type=MESH)
    pl.semaphore_wait(sem, len(devices))


def remote(src, dst, send, recv, device):
    return pltpu.make_async_remote_copy(
        src_ref=src, dst_ref=dst, send_sem=send, recv_sem=recv, device_id=device, device_id_type=MESH
    )


def cols(start, width):
    return pl.ds(pl.multiple_of(start, 128), width)


def ring_field(ring, x2d, w_hbm, wbuf, wsem, part, recv, gath, rs_sem, ag_sem, ssem, finish, consume):
    n = ring.n
    h = part.shape[2]
    nt = wbuf.shape[2]
    tiles = h // nt
    w = nt // 2
    last = 2 * n - 2

    def load(t):
        return pltpu.make_async_copy(
            w_hbm.at[:, cols(t * nt, nt)], wbuf.at[lax.rem(t, 2)], wsem.at[lax.rem(t, 2)]
        )

    def rs(t, d, step):
        area = cols(t * nt + d * w, w)
        return remote(
            part.at[ring.rs_chunk(d, step), :, area],
            recv.at[step, :, area],
            ssem.at[t, d],
            rs_sem.at[t, d, step],
            ring.peer(d),
        )

    def ag(t, d, step):
        area = cols(t * nt + d * w, w)
        chunk = ring.ag_chunk(d, step)
        return remote(
            gath.at[chunk, :, area], gath.at[chunk, :, area], ssem.at[t, d], ag_sem.at[t, d, step], ring.peer(d)
        )

    def slot(k, carry):
        @pl.when(k < tiles)
        def _():
            load(k).wait()

            @pl.when(k + 1 < tiles)
            def _():
                load(k + 1).start()

            sub = min(nt, 256)

            def piece(i, c):
                value = jnp.dot(
                    x2d(), wbuf[lax.rem(k, 2), :, cols(i * sub, sub)], preferred_element_type=F32
                )
                part[:, :, cols(k * nt + i * sub, sub)] = value.astype(BF16).reshape(n, part.shape[1], sub)
                return c

            lax.fori_loop(0, nt // sub, piece, 0)
            for d in range(2):
                rs(k, d, 0).start()

        def tile(t, c):
            j = k - t

            @pl.when((j >= 1) & (j <= n - 2))
            def _():
                for d in range(2):
                    area = cols(t * nt + d * w, w)
                    rs(t, d, j - 1).wait()
                    q = ring.rs_chunk(d, j)
                    total = part[q, :, area].astype(F32) + recv[j - 1, :, area].astype(F32)
                    part[q, :, area] = total.astype(BF16)
                    rs(t, d, j).start()

            @pl.when(j == n - 1)
            def _():
                for d in range(2):
                    area = cols(t * nt + d * w, w)
                    rs(t, d, n - 2).wait()
                    total = part[ring.me, :, area].astype(F32) + recv[n - 2, :, area].astype(F32)
                    gath[ring.me, :, area] = finish(area, total)
                    ag(t, d, 0).start()

            @pl.when((j >= n) & (j <= 2 * n - 3))
            def _():
                for d in range(2):
                    ag(t, d, j - n).wait()
                    ag(t, d, j - n + 1).start()

            @pl.when(j == last)
            def _():
                for d in range(2):
                    ag(t, d, n - 2).wait()

            return c

        lax.fori_loop(jnp.maximum(k - last, 0), jnp.minimum(k + 1, tiles), tile, 0)
        if consume is not None:

            @pl.when(k == last - 1)
            def _():
                load(0).start()

            @pl.when(k >= last)
            def _():
                t = k - last
                load(t).wait()

                @pl.when(t + 1 < tiles)
                def _():
                    load(t + 1).start()

                consume(t)

        return carry

    lax.fori_loop(0, tiles + last, slot, 0)


def positive_kernel(
    n, m, vis, w_hbm, uni, bias, sample_out, probs_out, part2_out, vis_out,
    x, wbuf, part, recv, gath, acc, narrow, wsem, rs_sem, ag_sem, ssem, own_sem, gs, gr, fs, fr, out_sem,
):
    ring, group = Ring(n), Group(m)
    rows_c = x.shape[1]
    batch = m * rows_c
    v = x.shape[2]
    nt = wbuf.shape[2]
    pltpu.make_async_copy(w_hbm.at[:, cols(0, nt)], wbuf.at[0], wsem.at[0]).start()
    own = pltpu.make_async_copy(vis, x.at[group.me], own_sem)
    own.start()
    offsets = range(1, group.chips)
    barrier([ring.peer(0), ring.peer(1), group.partner] + [group.peer(o) for o in offsets])
    own.wait()
    sends = [
        remote(x.at[group.me], x.at[group.me], gs.at[o - 1], gr.at[o - 1], group.peer(o)) for o in offsets
    ]
    for copy in sends:
        copy.start()
    mine = remote(x.at[group.me], x.at[group.me], fs.at[0], fr.at[0], group.partner)
    mine.start()
    forwards = []
    for o in offsets:
        sends[o - 1].wait()
        block = 2 * group.chip_at(group.chips - o) + group.core
        copy = remote(x.at[block], x.at[block], fs.at[o], fr.at[o], group.partner)
        copy.start()
        forwards.append(copy)
    mine.wait()
    for copy in forwards:
        copy.wait()
    save_x = pltpu.make_async_copy(x, vis_out, out_sem.at[0])
    save_x.start()

    def x2d():
        return x[...].reshape(batch, v)

    def finish(area, total):
        field = total + bias[:, area]
        probs_out[:, area] = sigmoid(field).astype(BF16)
        sample = relaxed(field, uni[:, area]).astype(BF16)
        sample_out[:, area] = sample
        return sample

    sub = min(v, 256)

    def consume(t):
        def piece(i, c):
            left = gath[:, :, cols(t * nt, nt)].reshape(batch, nt)
            right = wbuf[lax.rem(t, 2), pl.ds(pl.multiple_of(i * sub, sub), sub), :]
            value = lax.dot_general(left, right, (((1,), (1,)), ((), ())), preferred_element_type=F32)
            area = cols(i * sub, sub)

            @pl.when(t == 0)
            def _():
                acc[:, area] = value

            @pl.when(t > 0)
            def _():
                acc[:, area] = acc[:, area] + value

            return c

        lax.fori_loop(0, v // sub, piece, 0)

    ring_field(ring, x2d, w_hbm, wbuf, wsem, part, recv, gath, rs_sem, ag_sem, ssem, finish, consume)
    save_x.wait()

    def shrink(i, c):
        area = cols(i * sub, sub)
        narrow[:, :, area] = acc[:, area].astype(BF16).reshape(m, rows_c, sub)
        return c

    lax.fori_loop(0, v // sub, shrink, 0)
    save = pltpu.make_async_copy(narrow, part2_out, out_sem.at[1])
    save.start()
    save.wait()


def reconstruct_kernel(
    n, m, part2, uni, bias, probs, recon_out, full_out, probs_out,
    pair, chip_sum, yrecv, rec, gp, ds, dr, ys, yr, gs, gr, ms, mr, fs, fr, ag_sem, ssem, own_sem, out_sem,
):
    ring, group = Ring(n), Group(m)
    rows_c, v = part2.shape[1], part2.shape[2]
    h = gp.shape[2]
    chips = group.chips
    offsets = range(1, chips)
    tiles = dr.shape[0]
    cw = v // tiles
    rtiles = ag_sem.shape[0]
    rnt = h // rtiles
    rw = rnt // 2
    own = pltpu.make_async_copy(probs, gp.at[ring.me], own_sem)
    own.start()
    barrier([ring.peer(0), ring.peer(1), group.partner] + [group.peer(o) for o in offsets])

    def pair_copy(t, y):
        area = cols(t * cw, cw)
        return remote(
            part2.at[2 * y + 1 - group.core, :, area], pair.at[y, :, area], ds.at[t, y], dr.at[t, y], group.partner
        )

    def y_copy(t, o):
        area = cols(t * cw, cw)
        return remote(chip_sum.at[o - 1, :, area], yrecv.at[o - 1, :, area], ys.at[t, o - 1], yr.at[t, o - 1], group.peer(o))

    def g_copy(t, o):
        area = cols(t * cw, cw)
        return remote(
            rec.at[group.me, :, area], rec.at[group.me, :, area], gs.at[t, o - 1], gr.at[t, o - 1], group.peer(o)
        )

    def m_copy(t):
        area = cols(t * cw, cw)
        return remote(rec.at[group.me, :, area], rec.at[group.me, :, area], ms.at[t], mr.at[t], group.partner)

    def f_copy(t, o):
        area = cols(t * cw, cw)
        block = 2 * group.chip_at(chips - o) + group.core
        return remote(rec.at[block, :, area], rec.at[block, :, area], fs.at[t, o - 1], fr.at[t, o - 1], group.partner)

    def ag(t, d, step):
        area = cols(t * rnt + d * rw, rw)
        chunk = ring.ag_chunk(d, step)
        return remote(gp.at[chunk, :, area], gp.at[chunk, :, area], ssem.at[t, d], ag_sem.at[t, d, step], ring.peer(d))

    def pairs(t, c):
        for y in range(chips):
            pair_copy(t, y).start()
        return c

    lax.fori_loop(0, tiles, pairs, 0)
    own.wait()

    def slot(k, carry):
        @pl.when(k < rtiles)
        def _():
            for d in range(2):
                ag(k, d, 0).start()

        @pl.when(k < tiles)
        def _():
            area = cols(k * cw, cw)
            for y in range(chips):
                pair_copy(k, y).wait()
            for o in offsets:
                y = group.chip_at(o)
                total = part2[2 * y + group.core, :, area].astype(F32) + pair[y, :, area].astype(F32)
                chip_sum[o - 1, :, area] = total.astype(BF16)
                y_copy(k, o).start()

        @pl.when((k >= 2) & (k < tiles + 2))
        def _():
            t = k - 2
            area = cols(t * cw, cw)
            total = part2[group.me, :, area].astype(F32) + pair[group.chip, :, area].astype(F32)
            for o in offsets:
                y_copy(t, o).wait()
                total = total + yrecv[o - 1, :, area].astype(F32)
            sample = relaxed(total + bias[:, area], uni[:, area]).astype(BF16)
            recon_out[:, area] = sample
            rec[group.me, :, area] = sample
            for o in offsets:
                g_copy(t, o).start()
            m_copy(t).start()

        @pl.when(k >= 4)
        def _():
            t = k - 4

            @pl.when(t < tiles)
            def _():
                for o in offsets:
                    g_copy(t, o).wait()
                    f_copy(t, o).start()

        def row_tile(t, c):
            j = k - t

            @pl.when((j >= 1) & (j <= n - 2))
            def _():
                for d in range(2):
                    ag(t, d, j - 1).wait()
                    ag(t, d, j).start()

            @pl.when(j == n - 1)
            def _():
                for d in range(2):
                    ag(t, d, n - 2).wait()

            return c

        lax.fori_loop(jnp.maximum(k - (n - 1), 0), jnp.minimum(k + 1, rtiles), row_tile, 0)
        return carry

    lax.fori_loop(0, max(tiles + 4, rtiles + n - 1), slot, 0)
    save_probs = pltpu.make_async_copy(gp, probs_out, out_sem.at[0])
    save_probs.start()

    def drain(t, c):
        m_copy(t).wait()
        for o in offsets:
            f_copy(t, o).wait()
        return c

    lax.fori_loop(0, tiles, drain, 0)
    save_full = pltpu.make_async_copy(rec, full_out, out_sem.at[1])
    save_full.start()
    save_probs.wait()
    save_full.wait()


def negative_kernel(
    n, x, w_hbm, bias, probs_out,
    wbuf, part, recv, gath, wsem, rs_sem, ag_sem, ssem, out_sem,
):
    ring = Ring(n)
    nt = wbuf.shape[2]
    pltpu.make_async_copy(w_hbm.at[:, cols(0, nt)], wbuf.at[0], wsem.at[0]).start()
    barrier([ring.peer(0), ring.peer(1)])

    def finish(area, total):
        return sigmoid(total + bias[:, area]).astype(BF16)

    ring_field(
        ring, lambda: x[...], w_hbm, wbuf, wsem, part, recv, gath, rs_sem, ag_sem, ssem, finish, None
    )
    save = pltpu.make_async_copy(gath, probs_out, out_sem)
    save.start()
    save.wait()


def params(cid):
    return pltpu.CompilerParams(collective_id=cid, has_side_effects=True, vmem_limit_bytes=LIMIT)


def ring_scratch(n, batch, v, h, nt):
    rows = batch // n
    return [
        pltpu.VMEM((2, v, nt), BF16),
        pltpu.VMEM((n, rows, h), BF16),
        pltpu.VMEM((n - 1, rows, h), BF16),
        pltpu.VMEM((n, rows, h), BF16),
    ]


def ring_sems(n, tiles):
    dma = pltpu.SemaphoreType.DMA
    return [dma((2,)), dma((tiles, 2, n - 1)), dma((tiles, 2, n - 1)), dma((tiles, 2))]


def on_device(visible_data, hidden_uniform, visible_uniform, weights, visible_bias, hidden_bias):
    n, m = lax.axis_size("row"), lax.axis_size("col")
    v, h = weights.shape
    rows_c, rows_r = visible_data.shape[0], hidden_uniform.shape[0]
    batch = rows_c * m
    chips = m // 2
    dma = pltpu.SemaphoreType.DMA
    shape = jax.ShapeDtypeStruct
    hbias, vbias = hidden_bias.reshape(1, h), visible_bias.reshape(1, v)
    nt = col_tile(h, 512)
    tiles = h // nt

    sample_own, probs_own, part2, visible_full = pl.pallas_call(
        functools.partial(positive_kernel, n, m),
        name="positive",
        out_shape=[
            shape((rows_r, h), BF16),
            shape((rows_r, h), BF16),
            shape((m, rows_c, v), BF16),
            shape((m, rows_c, v), BF16),
        ],
        in_specs=[ANY, ANY, VM, VM],
        out_specs=[VM, VM, ANY, ANY],
        scratch_shapes=[pltpu.VMEM((m, rows_c, v), BF16)]
        + ring_scratch(n, batch, v, h, nt)
        + [pltpu.VMEM((batch, v), F32), pltpu.VMEM((m, rows_c, v), BF16)]
        + ring_sems(n, tiles)
        + [dma, dma((max(chips - 1, 1),)), dma((max(chips - 1, 1),)), dma((chips,)), dma((chips,)), dma((2,))],
        compiler_params=params(1),
        cost_estimate=pl.CostEstimate(flops=4 * batch * v * h, bytes_accessed=4 * v * h, transcendentals=0),
    )(visible_data, weights, hidden_uniform, hbias)

    cw = col_tile(v, 512)
    vtiles = v // cw
    rtiles = max(1, h // 1024)
    recon_own, recon_full, probs_full = pl.pallas_call(
        functools.partial(reconstruct_kernel, n, m),
        name="reconstruct",
        out_shape=[shape((rows_c, v), BF16), shape((m, rows_c, v), BF16), shape((n, rows_r, h), BF16)],
        in_specs=[VM, VM, VM, ANY],
        out_specs=[VM, ANY, ANY],
        scratch_shapes=[
            pltpu.VMEM((chips, rows_c, v), BF16),
            pltpu.VMEM((max(chips - 1, 1), rows_c, v), BF16),
            pltpu.VMEM((max(chips - 1, 1), rows_c, v), BF16),
            pltpu.VMEM((m, rows_c, v), BF16),
            pltpu.VMEM((n, rows_r, h), BF16),
            dma((vtiles, chips)),
            dma((vtiles, chips)),
        ]
        + [dma((vtiles, max(chips - 1, 1)))] * 4
        + [dma((vtiles,))] * 2
        + [dma((vtiles, max(chips - 1, 1)))] * 2
        + [dma((rtiles, 2, n - 1)), dma((rtiles, 2)), dma, dma((2,))],
        compiler_params=params(2),
        cost_estimate=pl.CostEstimate(flops=2 * batch * v * h, bytes_accessed=8 * batch * v, transcendentals=0),
    )(part2, visible_uniform, vbias, probs_own)

    recon2d = recon_full.reshape(batch, v)
    negative_full = pl.pallas_call(
        functools.partial(negative_kernel, n),
        name="negative",
        out_shape=shape((n, rows_r, h), BF16),
        in_specs=[VM, ANY, VM],
        out_specs=ANY,
        scratch_shapes=ring_scratch(n, batch, v, h, nt) + ring_sems(n, tiles) + [dma],
        compiler_params=params(3),
        cost_estimate=pl.CostEstimate(flops=2 * batch * v * h, bytes_accessed=2 * v * h, transcendentals=0),
    )(recon2d, weights, hbias)

    visible_full = visible_full.reshape(batch, v)
    probs_full, negative_full = probs_full.reshape(batch, h), negative_full.reshape(batch, h)
    left_side = jnp.concatenate([visible_full, recon2d], axis=0)
    right_side = jnp.concatenate([probs_full, -negative_full], axis=0)
    difference = lax.dot_general(
        left_side, right_side, (((0,), (0,)), ((), ())), preferred_element_type=F32
    )
    grad_weights = (difference / batch).astype(BF16)
    grad_visible = jnp.mean(visible_full.astype(F32) - recon2d.astype(F32), axis=0)
    grad_hidden = jnp.mean(probs_full.astype(F32) - negative_full.astype(F32), axis=0)
    return (grad_weights, grad_visible, grad_hidden, sample_own, recon_own)


def solution(mesh):
    placed = (
        P("col", "row"),
        P("row", "col"),
        P("col", "row"),
        P("row", "col"),
        P("row"),
        P("col"),
    )
    return jax.shard_map(
        on_device,
        mesh=mesh,
        in_specs=placed,
        out_specs=(P("row", "col"), P("row"), P("col"), P("row", "col"), P("col", "row")),
        check_vma=False,
    )
```

```python
import functools

import jax
import jax.numpy as jnp
from jax import lax
from jax.experimental import pallas as pl
from jax.experimental.pallas import tpu as pltpu
from jax.sharding import PartitionSpec as P

MESH = pl.DeviceIdType.MESH
BF16 = jnp.bfloat16
F32 = jnp.float32
ANY = pl.BlockSpec(memory_space=pl.ANY)
VM = pl.BlockSpec(memory_space=pltpu.VMEM)
LIMIT = 64_000_000


def sigmoid(t):
    return 1.0 / (1.0 + jnp.exp(-t))


def relaxed(field, uniform):
    return sigmoid(2.0 * (field + jnp.log(uniform) - jnp.log(1.0 - uniform)))


def col_tile(size, want):
    return min(size, want)


class Ring:
    def __init__(self, n):
        self.n = n
        me = lax.axis_index("row")
        self.me = me
        self.col = lax.axis_index("col")
        half, odd = me // 2, me % 2
        self.pos = half + odd * (n - 1 - 2 * half)
        self.right = self.index(self.pos + 1)
        self.left = self.index(self.pos + n - 1)

    def index(self, p):
        p = lax.rem(p, self.n)
        far = p // (self.n // 2)
        return (1 - far) * (2 * p) + far * (2 * (self.n - 1 - p) + 1)

    def peer(self, d):
        return (self.right if d == 0 else self.left, self.col)

    def rs_chunk(self, d, step):
        if d == 0:
            return self.index(self.pos + 2 * self.n - 1 - step)
        return self.index(self.pos + 1 + step)

    def ag_chunk(self, d, step):
        if d == 0:
            return self.index(self.pos + self.n - step)
        return self.index(self.pos + step)


class Group:
    def __init__(self, m):
        self.m = m
        self.chips = m // 2
        self.me = lax.axis_index("col")
        self.row = lax.axis_index("row")
        self.chip, self.core = self.me // 2, self.me % 2
        self.partner = (self.row, 2 * self.chip + 1 - self.core)

    def chip_at(self, offset):
        return lax.rem(self.chip + offset, self.chips)

    def peer(self, offset):
        return (self.row, 2 * self.chip_at(offset) + self.core)


def barrier(devices):
    sem = pltpu.get_barrier_semaphore()
    for device in devices:
        pl.semaphore_signal(sem, inc=1, device_id=device, device_id_type=MESH)
    pl.semaphore_wait(sem, len(devices))


def remote(src, dst, send, recv, device):
    return pltpu.make_async_remote_copy(
        src_ref=src, dst_ref=dst, send_sem=send, recv_sem=recv, device_id=device, device_id_type=MESH
    )


def cols(start, width):
    return pl.ds(pl.multiple_of(start, 128), width)


def add_rows(total, area, block):
    total[:, area] = total[:, area] + jnp.sum(block.astype(F32), axis=0, keepdims=True)


class RingSum:
    def __init__(self, ring, part, recv, gath, rs_sem, ag_sem, ssem):
        self.ring, self.part, self.recv, self.gath = ring, part, recv, gath
        self.rs_sem, self.ag_sem, self.ssem = rs_sem, ag_sem, ssem
        self.tiles = ssem.shape[0]
        self.half = part.shape[2] // 2
        self.w = self.half // self.tiles

    def area(self, t, d):
        return cols(d * self.half + t * self.w, self.w)

    def rs(self, t, d, step):
        area, ring = self.area(t, d), self.ring
        return remote(
            self.part.at[ring.rs_chunk(d, step), :, area],
            self.recv.at[step, :, area],
            self.ssem.at[t, d],
            self.rs_sem.at[t, d, step],
            ring.peer(d),
        )

    def ag(self, t, d, step):
        area, ring = self.area(t, d), self.ring
        block = self.gath.at[ring.ag_chunk(d, step), :, area]
        return remote(block, block, self.ssem.at[t, d], self.ag_sem.at[t, d, step], ring.peer(d))

    def each(self, body):
        def tile(t, c):
            for d in range(2):
                body(t, d, self.area(t, d))
            return c

        lax.fori_loop(0, self.tiles, tile, 0)

    def reduce(self, finish):
        ring, part, recv, gath = self.ring, self.part, self.recv, self.gath
        n = ring.n

        def step(j, c):
            def body(t, d, area):
                self.rs(t, d, j - 1).wait()
                q = ring.rs_chunk(d, j)
                total = part[q, :, area].astype(F32) + recv[j - 1, :, area].astype(F32)
                part[q, :, area] = total.astype(BF16)
                self.rs(t, d, j).start()

            self.each(body)
            return c

        lax.fori_loop(1, n - 1, step, 0)

        def close(t, d, area):
            self.rs(t, d, n - 2).wait()
            total = part[ring.me, :, area].astype(F32) + recv[n - 2, :, area].astype(F32)
            gath[ring.me, :, area] = finish(area, total)
            self.ag(t, d, 0).start()

        self.each(close)

    def gather(self, arrived, between):
        n = self.ring.n

        def step(s, c):
            def body(t, d, area):
                self.ag(t, d, s).wait()
                self.ag(t, d, s + 1).start()
                if arrived is not None:
                    arrived(area, self.gath[self.ring.ag_chunk(d, s + 1), :, area])

            self.each(body)
            if between is not None:
                between(s)
            return c

        lax.fori_loop(0, n - 2, step, 0)

        def close(t, d, area):
            self.ag(t, d, n - 2).wait()
            if arrived is not None:
                arrived(area, self.gath[self.ring.ag_chunk(d, n - 1), :, area])

        self.each(close)


PIECES = 4


def positive_kernel(
    n, m, vis, w_hbm, uni, bias, sample_out, probs_out, vsum_out, part2_out, vis_out,
    x, wbuf, part, recv, gath, acc, narrow, wsem, rs_sem, ag_sem, ssem, own_sem, gs, gr, fs, fr, ms, mr, out_sem,
):
    ring, group = Ring(n), Group(m)
    rows_c, rows_r = x.shape[1], part.shape[1]
    v, h = x.shape[2], part.shape[2]
    vb = v // PIECES
    chips = group.chips
    pair = 2 * rows_c
    chunks = pair // rows_r
    offsets = range(1, chips)
    sub = min(vb, h, 256)

    def load(i):
        block = lax.rem(i, PIECES)
        return pltpu.make_async_copy(
            w_hbm.at[pl.ds(pl.multiple_of(block * vb, vb), vb), :], wbuf.at[lax.rem(i, 2)], wsem.at[lax.rem(i, 2)]
        )

    load(0).start()
    load(1).start()
    own = pltpu.make_async_copy(vis, x.at[group.me], own_sem)
    own.start()
    barrier([ring.peer(0), ring.peer(1), group.partner] + [group.peer(o) for o in offsets])
    own.wait()

    def y_copy(o, p):
        block = x.at[group.me, :, cols(p * vb, vb)]
        return remote(block, block, gs.at[o - 1, p], gr.at[o - 1, p], group.peer(o))

    def f_copy(o, p):
        block = x.at[2 * group.chip_at(chips - o) + group.core, :, cols(p * vb, vb)]
        return remote(block, block, fs.at[o - 1, p], fr.at[o - 1, p], group.partner)

    mine = remote(x.at[group.me], x.at[group.me], ms, mr, group.partner)
    mine.start()
    for p in range(PIECES):
        for o in offsets:
            y_copy(o, p).start()

    sums = RingSum(ring, part, recv, gath, rs_sem, ag_sem, ssem)

    def dot_piece(chip, p, i, width, after):
        rows = pl.ds(pl.multiple_of(chip * pair, pair), pair)

        def piece(start):
            left = x[pl.ds(2 * chip, 2), :, cols(p * vb, vb)].reshape(pair, vb)
            value = jnp.dot(left, wbuf[i % 2, :, cols(start, sub)], preferred_element_type=F32)
            area = cols(start, sub)
            if p > 0:
                value = value + acc[rows, area]
            if p < PIECES - 1:
                acc[rows, area] = value
            else:
                part[pl.ds(chip * chunks, chunks), :, area] = value.astype(BF16).reshape(chunks, rows_r, sub)

        def tile(t, c):
            for d in range(2):

                def one(g, e):
                    piece(d * sums.half + t * width + g * sub)
                    return e

                lax.fori_loop(0, width // sub, one, 0)
                if after:
                    sums.rs(t, d, 0).start()
            return c

        lax.fori_loop(0, sums.half // width, tile, 0)

    mine.wait()
    for p in range(PIECES):
        load(p).wait()
        dot_piece(group.chip, p, p, sums.w, False)
        load(p + 2).start()
        if p == 1:
            for o in offsets:
                y_copy(o, 0).wait()
                f_copy(o, 0).start()
    for p in range(PIECES):
        if p + 1 < PIECES:
            for o in offsets:
                y_copy(o, p + 1).wait()
                f_copy(o, p + 1).start()
        i = PIECES + p
        load(i).wait()
        for o in offsets:
            f_copy(o, p).wait()
            dot_piece(group.chip_at(chips - o), p, i, sums.w, p == PIECES - 1 and o == chips - 1)
        load(i + 2).start()
    save_x = pltpu.make_async_copy(x, vis_out, out_sem.at[0])
    save_x.start()

    vsub = min(v, 256)

    def clear(i, c):
        area = cols(i * vsub, vsub)
        acc[:, area] = jnp.zeros((acc.shape[0], vsub), F32)
        vsum_out[:, area] = jnp.sum(x[:, :, area].astype(F32).reshape(m * rows_c, vsub), axis=0, keepdims=True)
        return c

    lax.fori_loop(0, v // vsub, clear, 0)

    def finish(area, total):
        field = total + bias[:, area]
        probs_out[:, area] = sigmoid(field).astype(BF16)
        sample = relaxed(field, uni[:, area]).astype(BF16)
        sample_out[:, area] = sample
        return sample

    many = n // 2

    def second(block, slot, base):
        psub = min(vb, 256)

        def piece(g, c):
            for d in range(2):
                ids = [ring.ag_chunk(d, base + i) for i in range(many)]
                k = pl.ds(d * sums.half, sums.half)
                left = jnp.concatenate([gath[q, :, k] for q in ids], axis=0)
                right = wbuf[slot, pl.ds(pl.multiple_of(g * psub, psub), psub), k]
                value = lax.dot_general(left, right, (((1,), (1,)), ((), ())), preferred_element_type=F32)
                area = cols(block * vb + g * psub, psub)
                for i, q in enumerate(ids):
                    rows = pl.ds(pl.multiple_of(q * rows_r, rows_r), rows_r)
                    acc[rows, area] = acc[rows, area] + value[i * rows_r : (i + 1) * rows_r, :]
            return c

        lax.fori_loop(0, vb // psub, piece, 0)

    def between(s):
        i = s - (many - 2)

        @pl.when((i >= 0) & (i < PIECES))
        def _():
            load(i).wait()
            second(i, lax.rem(i, 2), 0)
            load(i + 2).start()

    sums.reduce(finish)
    sums.gather(None, between)

    def save(i):
        area = cols(i * vb, vb)
        return pltpu.make_async_copy(narrow.at[:, :, area], part2_out.at[:, :, area], out_sem.at[1 + i])

    for i in range(PIECES):
        load(i).wait()
        second(i, i % 2, many)
        if i + 2 < PIECES:
            load(i + 2).start()

        def shrink(g, c):
            area = cols(i * vb + g * sub, sub)
            narrow[:, :, area] = acc[:, area].astype(BF16).reshape(m, rows_c, sub)
            return c

        lax.fori_loop(0, vb // sub, shrink, 0)
        save(i).start()
    save_x.wait()
    for i in range(PIECES):
        save(i).wait()


def negative_kernel(
    n, m, part2, uni, bias, hbias, vsum, probs, w_hbm, recon_out, gv_out, gh_out, full_out, probs_out, neg_out,
    pair, chip_sum, yrecv, rec, gp, wbuf, acc, part, recv, gath, hsum, rsum,
    ds, dr, ys, yr, gs, gr, fs, fr, ms, mr, agp_sem, agp_send, wsem, rs_sem, ag_sem, ssem, own_sem, out_sem,
):
    ring, group = Ring(n), Group(m)
    rows_c, v = part2.shape[1], part2.shape[2]
    rows_r, h = gp.shape[1], gp.shape[2]
    batch = m * rows_c
    chips = group.chips
    offsets = range(1, chips)
    tiles = dr.shape[0]
    cw = v // tiles
    rtiles = agp_sem.shape[0]
    rnt = h // rtiles
    rw = rnt // 2
    own = pltpu.make_async_copy(probs, gp.at[ring.me], own_sem)
    own.start()

    def load(t):
        return pltpu.make_async_copy(
            w_hbm.at[pl.ds(pl.multiple_of(t * cw, cw), cw), :], wbuf.at[lax.rem(t, 2)], wsem.at[lax.rem(t, 2)]
        )

    load(0).start()
    barrier([ring.peer(0), ring.peer(1), group.partner] + [group.peer(o) for o in offsets])

    def pair_copy(t, y):
        area = cols(t * cw, cw)
        return remote(
            part2.at[2 * y + 1 - group.core, :, area], pair.at[y, :, area], ds.at[t, y], dr.at[t, y], group.partner
        )

    def y_copy(t, o):
        area = cols(t * cw, cw)
        return remote(
            chip_sum.at[o - 1, :, area], yrecv.at[o - 1, :, area], ys.at[t, o - 1], yr.at[t, o - 1], group.peer(o)
        )

    def g_copy(t, o):
        block = rec.at[group.me, :, cols(t * cw, cw)]
        return remote(block, block, gs.at[t, o - 1], gr.at[t, o - 1], group.peer(o))

    def m_copy(t):
        block = rec.at[group.me, :, cols(t * cw, cw)]
        return remote(block, block, ms.at[t], mr.at[t], group.partner)

    def f_copy(t, o):
        block = rec.at[2 * group.chip_at(chips - o) + group.core, :, cols(t * cw, cw)]
        return remote(block, block, fs.at[t, o - 1], fr.at[t, o - 1], group.partner)

    def ag(t, d, step):
        block = gp.at[ring.ag_chunk(d, step), :, cols(t * rnt + d * rw, rw)]
        return remote(block, block, agp_send.at[t, d], agp_sem.at[t, d, step], ring.peer(d))

    def pairs(t, c):
        for y in range(chips):
            pair_copy(t, y).start()
        return c

    lax.fori_loop(0, tiles, pairs, 0)
    own.wait()
    hsum[...] = jnp.zeros_like(hsum)
    rsum[...] = jnp.zeros_like(rsum)
    sub = min(h, 256)

    def slot(k, carry):
        @pl.when(k < rtiles)
        def _():
            for d in range(2):
                ag(k, d, 0).start()
                area = cols(k * rnt + d * rw, rw)
                add_rows(hsum, area, gp[ring.me, :, area])

        @pl.when(k < tiles)
        def _():
            area = cols(k * cw, cw)
            for y in range(chips):
                pair_copy(k, y).wait()
            for o in offsets:
                y = group.chip_at(o)
                total = part2[2 * y + group.core, :, area].astype(F32) + pair[y, :, area].astype(F32)
                chip_sum[o - 1, :, area] = total.astype(BF16)
                y_copy(k, o).start()

        @pl.when((k >= 2) & (k < tiles + 2))
        def _():
            t = k - 2
            area = cols(t * cw, cw)
            total = part2[group.me, :, area].astype(F32) + pair[group.chip, :, area].astype(F32)
            for o in offsets:
                y_copy(t, o).wait()
                total = total + yrecv[o - 1, :, area].astype(F32)
            sample = relaxed(total + bias[:, area], uni[:, area]).astype(BF16)
            recon_out[:, area] = sample
            rec[group.me, :, area] = sample
            for o in offsets:
                g_copy(t, o).start()
            m_copy(t).start()

        @pl.when((k >= 4) & (k < tiles + 4))
        def _():
            for o in offsets:
                g_copy(k - 4, o).wait()
                f_copy(k - 4, o).start()

        def row_tile(t, c):
            j = k - t
            for d in range(2):
                area = cols(t * rnt + d * rw, rw)

                @pl.when(j >= 1)
                def _():
                    ag(t, d, j - 1).wait()

                    @pl.when(j <= n - 2)
                    def _():
                        ag(t, d, j).start()

                    add_rows(hsum, area, gp[ring.ag_chunk(d, j), :, area])

            return c

        lax.fori_loop(jnp.maximum(k - (n - 1), 0), jnp.minimum(k + 1, rtiles), row_tile, 0)

        @pl.when((k >= 5) & (k < tiles + 5))
        def _():
            t = k - 5
            area = cols(t * cw, cw)

            @pl.when(t + 1 < tiles)
            def _():
                load(t + 1).start()

            m_copy(t).wait()
            for o in offsets:
                f_copy(t, o).wait()
            load(t).wait()

            def piece(g, c):
                out = cols(g * sub, sub)
                left = rec[:, :, area].reshape(batch, cw)
                value = jnp.dot(left, wbuf[lax.rem(t, 2), :, out], preferred_element_type=F32)

                @pl.when(t == 0)
                def _():
                    acc[:, out] = value

                @pl.when(t > 0)
                def _():
                    acc[:, out] = acc[:, out] + value

                return c

            lax.fori_loop(0, h // sub, piece, 0)
            add_rows(rsum, area, rec[:, :, area].reshape(batch, cw))

        return carry

    lax.fori_loop(0, max(tiles + 5, rtiles + n - 1), slot, 0)

    sums = RingSum(ring, part, recv, gath, rs_sem, ag_sem, ssem)

    def begin(t, d, area):
        part[:, :, area] = acc[:, area].astype(BF16).reshape(n, rows_r, sums.w)
        sums.rs(t, d, 0).start()

    sums.each(begin)
    save_probs = pltpu.make_async_copy(gp, probs_out, out_sem.at[0])
    save_probs.start()
    save_full = pltpu.make_async_copy(rec, full_out, out_sem.at[1])
    save_full.start()
    gv_out[...] = (vsum[...] - rsum[...]) * (1.0 / batch)

    def finish(area, total):
        value = -sigmoid(total + hbias[:, area]).astype(BF16)
        add_rows(hsum, area, value)
        return value

    def arrived(area, block):
        add_rows(hsum, area, block)

    sums.reduce(finish)
    sums.gather(arrived, None)
    save_neg = pltpu.make_async_copy(gath, neg_out, out_sem.at[2])
    save_neg.start()
    gh_out[...] = hsum[...] * (1.0 / batch)
    save_probs.wait()
    save_full.wait()
    save_neg.wait()


def params(cid):
    return pltpu.CompilerParams(collective_id=cid, has_side_effects=True, vmem_limit_bytes=LIMIT)


def on_device(visible_data, hidden_uniform, visible_uniform, weights, visible_bias, hidden_bias):
    n, m = lax.axis_size("row"), lax.axis_size("col")
    v, h = weights.shape
    rows_c, rows_r = visible_data.shape[0], hidden_uniform.shape[0]
    batch = rows_c * m
    chips = m // 2
    others = max(chips - 1, 1)
    dma = pltpu.SemaphoreType.DMA
    shape = jax.ShapeDtypeStruct
    hbias, vbias = hidden_bias.reshape(1, h), visible_bias.reshape(1, v)
    tiles = (h // 2) // col_tile(h // 2, 512)
    by_row, by_col = (n, rows_r, h), (m, rows_c, v)
    ring_buffers = [pltpu.VMEM(by_row, BF16), pltpu.VMEM((n - 1, rows_r, h), BF16), pltpu.VMEM(by_row, BF16)]
    ring_sems = [dma((tiles, 2, n - 1)), dma((tiles, 2, n - 1)), dma((tiles, 2))]

    sample_own, probs_own, vsum, part2, visible_full = pl.pallas_call(
        functools.partial(positive_kernel, n, m),
        name="positive",
        out_shape=[
            shape((rows_r, h), BF16),
            shape((rows_r, h), BF16),
            shape((1, v), F32),
            shape(by_col, BF16),
            shape(by_col, BF16),
        ],
        in_specs=[ANY, ANY, VM, VM],
        out_specs=[VM, VM, VM, ANY, ANY],
        scratch_shapes=[pltpu.VMEM(by_col, BF16), pltpu.VMEM((2, v // PIECES, h), BF16)]
        + ring_buffers
        + [pltpu.VMEM((batch, max(v, h)), F32), pltpu.VMEM(by_col, BF16), dma((2,))]
        + ring_sems
        + [dma]
        + [dma((others, PIECES))] * 4
        + [dma, dma, dma((1 + PIECES,))],
        compiler_params=params(1),
        cost_estimate=pl.CostEstimate(flops=4 * batch * v * h, bytes_accessed=8 * v * h, transcendentals=0),
    )(visible_data, weights, hidden_uniform, hbias)

    cw = col_tile(v, 512)
    vtiles = v // cw
    rtiles = max(1, h // 1024)
    recon_own, grad_visible, grad_hidden, recon_full, probs_full, negative_full = pl.pallas_call(
        functools.partial(negative_kernel, n, m),
        name="negative",
        out_shape=[
            shape((rows_c, v), BF16),
            shape((1, v), F32),
            shape((1, h), F32),
            shape(by_col, BF16),
            shape(by_row, BF16),
            shape(by_row, BF16),
        ],
        in_specs=[VM, VM, VM, VM, VM, ANY, ANY],
        out_specs=[VM, VM, VM, ANY, ANY, ANY],
        scratch_shapes=[
            pltpu.VMEM((chips, rows_c, v), BF16),
            pltpu.VMEM((others, rows_c, v), BF16),
            pltpu.VMEM((others, rows_c, v), BF16),
            pltpu.VMEM(by_col, BF16),
            pltpu.VMEM(by_row, BF16),
            pltpu.VMEM((2, cw, h), BF16),
            pltpu.VMEM((batch, h), F32),
        ]
        + ring_buffers
        + [pltpu.VMEM((1, h), F32), pltpu.VMEM((1, v), F32)]
        + [dma((vtiles, chips))] * 2
        + [dma((vtiles, others))] * 6
        + [dma((vtiles,))] * 2
        + [dma((rtiles, 2, n - 1)), dma((rtiles, 2)), dma((2,))]
        + ring_sems
        + [dma, dma((3,))],
        compiler_params=params(2),
        cost_estimate=pl.CostEstimate(flops=2 * batch * v * h, bytes_accessed=2 * v * h, transcendentals=0),
    )(part2, visible_uniform, vbias, hbias, vsum, probs_own, weights)

    left_side = jnp.concatenate([visible_full, recon_full], axis=0).reshape(2 * batch, v)
    right_side = jnp.concatenate([probs_full, negative_full], axis=0).reshape(2 * batch, h)
    difference = lax.dot_general(
        left_side, right_side, (((0,), (0,)), ((), ())), preferred_element_type=F32
    )
    grad_weights = (difference / batch).astype(BF16)
    return (grad_weights, grad_visible.reshape(v), grad_hidden.reshape(h), sample_own, recon_own)


def solution(mesh):
    placed = (
        P("col", "row"),
        P("row", "col"),
        P("col", "row"),
        P("row", "col"),
        P("row"),
        P("col"),
    )
    return jax.shard_map(
        on_device,
        mesh=mesh,
        in_specs=placed,
        out_specs=(P("row", "col"), P("row"), P("col"), P("row", "col"), P("col", "row")),
        check_vma=False,
    )
```
